128 devices in a mesh: outer: 16 (over z_lo, x, core), inner: 8 (over y, z_hi).
Axes of the slice: x: 4, y: 4, z: 4 (z_hi: 2, z_lo: 2; z = z_hi * 2 + z_lo), core: 2. Of those that a mesh axis runs over, the one named last changes fastest.
Arguments:
- hidden: bfloat16 [16384, 4096], P(('outer', 'inner')), may hold values from -16 to 16
- position: int32 [16384], P(('outer', 'inner')), may hold values from 0 to 16383, as said below
- query_weight: bfloat16 [4096, 512], replicated, may hold values from -0.09375 to 0.09375
- key_weight: bfloat16 [4096, 128], replicated, may hold values from -0.09375 to 0.09375
- value_weight: bfloat16 [4096, 128], replicated, may hold values from -0.09375 to 0.09375
- output_grad: bfloat16 [16384, 512], P(('outer', 'inner')), may hold values from -6 to 6
Outputs:
- attended: bfloat16 [16384, 512], P(('outer', 'inner'))
- hidden_grad: bfloat16 [16384, 4096], P(('outer', 'inner'))
- query_weight_grad: float32 [4096, 512], P(('outer', 'inner'))
- key_weight_grad: float32 [4096, 128], P(('outer', 'inner'))
- value_weight_grad: float32 [4096, 128], P(('outer', 'inner'))
The draws below stay inside these ranges and needn't reach their ends.
Inputs may be any that keep to these rules, and one draw needn't show every extreme that they name: Each device's rows hold two runs of 64 consecutive positions in rising order: first the run that starts at a * 64, then the run that starts at (255 - a) * 64, for some a below 128 that differs from device to device; every position occurs once.
All inputs are finite; a program needn't handle non-finite values.
Results may differ from the reference program's by a relative error of at most 0.019.
The reference program's roundings to bfloat16 on the way count: a program that leaves them out, or rounds other values in their place, can miss the bound.
Values may be sent and summed in bfloat16 or wider, within the bound.
A program may use at most 128 MiB of HBM per device.

```python
import jax
import jax.numpy as jnp
import numpy as np
from jax import lax

D = 4096
HQ = 4
HD = 128
TOK_DEV = 128
HALF = 64
TOKENS = 16384
BLOCKS = 256


def draw_position(key, part):
    device_count = TOKENS // TOK_DEV
    pairings = jax.random.permutation(jax.random.fold_in(key, 11), device_count).astype(jnp.int32)
    offsets = jnp.arange(HALF, dtype=jnp.int32)
    low_run = pairings[:, None] * HALF + offsets[None, :]
    high_run = (BLOCKS - 1 - pairings)[:, None] * HALF + offsets[None, :]
    return jnp.concatenate([low_run, high_run], axis=1).reshape(TOKENS).astype(jnp.int32)


def draw_hidden(key, part):
    samples = jax.random.normal(jax.random.fold_in(key, 1), (TOKENS, D), jnp.float32)
    return jnp.clip(samples, -16.0, 16.0).astype(jnp.bfloat16)


def levels(own_key, extent, cuts, smallest, top_value):
    def one(dim, parts):
        draws = jax.random.uniform(jax.random.fold_in(jax.random.fold_in(own_key, 6), dim), (parts,), jnp.float32, smallest / len(cuts), top_value / len(cuts))
        return jnp.repeat(jnp.exp(draws), extent[dim] // parts).reshape((-1,) + (1,) * (len(extent) - dim - 1))

    factor_of = one(*cuts[0])
    for cut in cuts[1:]:
        factor_of = factor_of * one(*cut)
    return factor_of


def bell_draw(key, extent, deviation, most, cuts=(), kind=jnp.bfloat16):
    drawn = deviation * jax.random.normal(key, extent, jnp.float32)
    if cuts:
        drawn = drawn * levels(key, extent, cuts, -0.22, 0.18)
    return jnp.clip(drawn, -most, most).astype(kind)


def setup_inputs(seed: int = 0) -> dict:
    splits = jax.random.split(jax.random.key(seed), 7)
    hidden = draw_hidden(jax.random.fold_in(splits[6], 71), 0)
    position = draw_position(jax.random.fold_in(splits[6], 71), 0)
    query_weight = bell_draw(splits[2], (D, HQ * HD), D ** -0.5, 0.09375)
    key_weight = bell_draw(splits[3], (D, HD), D ** -0.5, 0.09375)
    value_weight = bell_draw(splits[4], (D, HD), D ** -0.5, 0.09375)
    output_grad = bell_draw(splits[5], (TOKENS, HQ * HD), 1.0, 6.0, ((0, 128),))
    return {"hidden": hidden, "position": position, "query_weight": query_weight, "key_weight": key_weight, "value_weight": value_weight, "output_grad": output_grad}


rope_theta = 500000.0
masked_score = -1.0e30
highest = lax.Precision.HIGHEST


def frequencies(head_width):
    exponents = np.arange(0, head_width, 2) / head_width
    plain_freq = rope_theta ** (-exponents)
    wavelength = 2.0 * np.pi / plain_freq
    blend = (8192.0 / wavelength - 1.0) / 3.0
    blended = (1.0 - blend) * plain_freq / 8.0 + blend * plain_freq
    scaled = np.where(wavelength > 8192.0, plain_freq / 8.0, np.where(wavelength < 2048.0, plain_freq, blended))
    return jnp.asarray(scaled, dtype=jnp.float32)


def rope_tables(position):
    angles = position.astype(jnp.float32)[:, None] * frequencies(HD)[None, :]
    return jnp.cos(angles), jnp.sin(angles)


def rotate(vector, cosine, sine_table):
    middle = vector.shape[-1] // 2
    leading = vector[..., :middle]
    trailing = vector[..., middle:]
    return jnp.concatenate([leading * cosine - trailing * sine_table, trailing * cosine + leading * sine_table], axis=-1)


def rotate_back(vector, cosine, sine_table):
    middle = vector.shape[-1] // 2
    leading = vector[..., :middle]
    trailing = vector[..., middle:]
    return jnp.concatenate([leading * cosine + trailing * sine_table, trailing * cosine - leading * sine_table], axis=-1)


def reference(hidden, position, query_weight, key_weight, value_weight, output_grad):
    tokens_all = hidden.shape[0]
    score_scale = float(HD) ** -0.5
    cosine, sine_table = rope_tables(position)
    query_proj = jnp.dot(hidden, query_weight, preferred_element_type=jnp.float32).reshape(tokens_all, HQ, HD)
    queries = rotate(query_proj, cosine[:, None, :], sine_table[:, None, :]).astype(jnp.bfloat16)
    rotated_keys = rotate(jnp.dot(hidden, key_weight, preferred_element_type=jnp.float32), cosine, sine_table).astype(jnp.bfloat16)
    value_rows = jnp.dot(hidden, value_weight, preferred_element_type=jnp.float32).astype(jnp.bfloat16)
    key_float = rotated_keys.astype(jnp.float32)
    value_float = value_rows.astype(jnp.float32)
    blocks = tokens_all // TOK_DEV
    query_blocks = queries.astype(jnp.float32).reshape(blocks, TOK_DEV, HQ, HD)
    grad_blocks = output_grad.astype(jnp.float32).reshape(blocks, TOK_DEV, HQ, HD)
    pos_blocks = position.reshape(blocks, TOK_DEV)

    def one_block(totals, inputs):
        key_total, value_total = totals
        query_block, grad_block, pos_block = inputs
        scores = jnp.einsum("qhd,kd->hqk", query_block, key_float, precision=highest) * score_scale
        allowed = position[None, None, :] <= pos_block[None, :, None]
        scores = jnp.where(allowed, scores, masked_score)
        row_max = jnp.max(scores, axis=2, keepdims=True)
        weights = jnp.where(allowed, jnp.exp(scores - row_max), 0.0)
        row_sum = jnp.sum(weights, axis=2, keepdims=True)
        probs_all = weights / row_sum
        probs_low = lax.optimization_barrier(probs_all.astype(jnp.bfloat16)).astype(jnp.float32)
        output = jnp.einsum("hqk,kd->qhd", probs_low, value_float, precision=highest)
        row_delta = jnp.sum(grad_block * output, axis=2)
        grad_probs = jnp.einsum("qhd,kd->hqk", grad_block, value_float, precision=highest)
        grad_scores = probs_all * (grad_probs - jnp.transpose(row_delta)[:, :, None])
        grad_low = lax.optimization_barrier(grad_scores.astype(jnp.bfloat16)).astype(jnp.float32)
        grad_query = jnp.einsum("hqk,kd->qhd", grad_low, key_float, precision=highest) * score_scale
        key_total = key_total + jnp.einsum("hqk,qhd->kd", grad_low, query_block, precision=highest) * score_scale
        value_total = value_total + jnp.einsum("hqk,qhd->kd", probs_low, grad_block, precision=highest)
        return (key_total, value_total), (output, grad_query)

    zeros = jnp.zeros((tokens_all, HD), jnp.float32)
    (key_total, value_total), (outputs, grad_queries) = lax.scan(one_block, (zeros, zeros), (query_blocks, grad_blocks, pos_blocks))
    attended = outputs.reshape(tokens_all, HQ * HD).astype(jnp.bfloat16)
    grad_q = rotate_back(grad_queries.reshape(tokens_all, HQ, HD), cosine[:, None, :], sine_table[:, None, :])
    grad_q = grad_q.reshape(tokens_all, HQ * HD).astype(jnp.bfloat16)
    grad_k = rotate_back(key_total, cosine, sine_table).astype(jnp.bfloat16)
    grad_v = value_total.astype(jnp.bfloat16)
    hidden_grad = jnp.dot(grad_q, query_weight.T, preferred_element_type=jnp.float32)
    hidden_grad = hidden_grad + jnp.dot(grad_k, key_weight.T, preferred_element_type=jnp.float32)
    hidden_grad = hidden_grad + jnp.dot(grad_v, value_weight.T, preferred_element_type=jnp.float32)
    hidden_grad = hidden_grad.astype(jnp.bfloat16)
    query_weight_grad = jnp.dot(hidden.T, grad_q, preferred_element_type=jnp.float32)
    key_weight_grad = jnp.dot(hidden.T, grad_k, preferred_element_type=jnp.float32)
    value_weight_grad = jnp.dot(hidden.T, grad_v, preferred_element_type=jnp.float32)
    return attended, hidden_grad, query_weight_grad, key_weight_grad, value_weight_grad
```

```python
import functools
import math

import jax
import jax.numpy as jnp
import numpy as np
from jax import lax
from jax.experimental import pallas as pl
from jax.experimental.pallas import tpu as pltpu
from jax.sharding import Mesh
from jax.sharding import PartitionSpec as P

HQ = 4
HD = 128
TOK = 128
CHIPS = 64
AXES = ("zl", "x", "c", "y", "zh")
ORDERS = (("x", "y", "z"), ("y", "z", "x"), ("z", "x", "y"))
MESH = pl.DeviceIdType.MESH
rope_theta = 500000.0
masked_score = -1e30
SCALE = float(HD) ** -0.5
LOG2E = math.log2(math.e)
VMEM_LIMIT = 64 * 1024 * 1024 - 131072
F32 = jnp.float32
BF16 = jnp.bfloat16


def frequencies(head_width):
    exponents = np.arange(0, head_width, 2) / head_width
    plain_freq = rope_theta ** (-exponents)
    wavelength = 2.0 * np.pi / plain_freq
    blend = (8192.0 / wavelength - 1.0) / 3.0
    blended = (1.0 - blend) * plain_freq / 8.0 + blend * plain_freq
    scaled = np.where(
        wavelength > 8192.0, plain_freq / 8.0, np.where(wavelength < 2048.0, plain_freq, blended)
    )
    return jnp.asarray(scaled, dtype=jnp.float32)


def here():
    zl, zh = lax.axis_index("zl"), lax.axis_index("zh")
    return {"x": lax.axis_index("x"), "y": lax.axis_index("y"), "z": zh * 2 + zl}


def along(axis, value):
    if axis == "z":
        return {"zl": value % 2, "zh": value // 2}
    return {axis: value}


def place(fixed):
    whole = slice(None)
    z = fixed.get("z")
    return (
        whole if z is None else z % 2,
        fixed.get("x", whole),
        fixed.get("y", whole),
        whole if z is None else z // 2,
    )


def left_dims(fixed):
    dims = []
    for name, size in (("z", 2), ("x", 4), ("y", 4), ("z", 2)):
        if name not in fixed:
            dims.append(size)
    return tuple(dims)


def enter(me, ring=True, partner=True):
    barrier = pltpu.get_barrier_semaphore()
    count = 0
    if ring:
        for axis in "xyz":
            for delta in (1, 3):
                pl.semaphore_signal(
                    barrier, inc=1, device_id=along(axis, (me[axis] + delta) % 4), device_id_type=MESH
                )
                count += 1
    if partner:
        pl.semaphore_signal(
            barrier, inc=1, device_id={"c": 1 - lax.axis_index("c")}, device_id_type=MESH
        )
        count += 1
    pl.semaphore_wait(barrier, count)


def remote(src, dst, sems, device_id):
    return pltpu.make_async_remote_copy(
        src_ref=src,
        dst_ref=dst,
        send_sem=sems[0],
        recv_sem=sems[1],
        device_id=device_id,
        device_id_type=MESH,
    )


def params(collective_id=None):
    if collective_id is None:
        return pltpu.CompilerParams(vmem_limit_bytes=VMEM_LIMIT)
    return pltpu.CompilerParams(
        collective_id=collective_id, has_side_effects=True, vmem_limit_bytes=VMEM_LIMIT
    )


def in_vmem(n):
    return [pl.BlockSpec(memory_space=pltpu.VMEM)] * n


KV_ROWS = TOK + 16
PART = KV_ROWS // 3


class Spread:
    def __init__(self, me, axis, spot, first, ref, send, recv, waits):
        self.me, self.axis, self.spot, self.first, self.ref = me, axis, spot, first, ref
        self.send, self.recv, self.waits = send, recv, waits

    def hop(self, slot, src, dst, delta):
        copy = remote(
            src,
            dst,
            (self.send.at[slot], self.recv.at[slot]),
            along(self.axis, (self.me[self.axis] + delta) % 4),
        )
        copy.start()
        self.waits.append(copy)
        return copy

    def start(self):
        dst = self.ref.at[self.spot(self.me[self.axis], slice(None))]
        src = dst if self.first is None else self.first
        self.near = (self.hop(0, src, dst, 1), self.hop(1, src, dst, 3))

    def forward(self):
        self.far = []
        for half, delta, origin in ((0, 1, 3), (1, 3, 1)):
            self.near[half].wait_recv()
            ref = self.ref.at[self.spot((self.me[self.axis] + origin) % 4, half)]
            self.far.append(self.hop(2 + half, ref, ref, delta))

    def finish(self):
        for copy in self.far:
            copy.wait_recv()


def gather_kernel(
    kv, q, do, tables, hid, kv_all, q_pair, do_pair, tables_pair, meta_pair, hid_partner,
    send, recv, pair_send, pair_recv,
):
    me = here()
    core = lax.axis_index("c")
    other = {"c": 1 - core}
    enter(me)
    pair, waits = [], []

    def to_partner(src, dst):
        n = len(pair)
        copy = remote(src, dst, (pair_send.at[n], pair_recv.at[n]), other)
        copy.start()
        pair.append(copy)

    def spread(k, ring, axis, fixed, first=None):
        rows = pl.ds(PART * k, PART)

        def spot(value, half):
            return (*place({**fixed, axis: value}), half, rows)

        return Spread(me, axis, spot, first, kv_all, send.at[k, ring], recv.at[k, ring], waits)

    lines, planes, spaces = [], [], []
    for k, (a, b, c) in enumerate(ORDERS):
        rows = pl.ds(PART * k, PART)
        lines.append(spread(k, 0, a, {b: me[b], c: me[c]}, kv.at[:, rows]))
        planes.append(spread(k, 1, b, {c: me[c]}))
        spaces.append(
            [spread(k, 2 + n, c, {b: (me[b] + off) % 4}) for n, off in enumerate((0, 3, 1, 2))]
        )

    for k in range(3):
        lines[k].start()
    kv_all[place(me)] = kv[...]
    to_partner(q, q_pair.at[core])
    to_partner(do, do_pair.at[core])
    to_partner(tables, tables_pair.at[core])
    to_partner(kv.at[0, pl.ds(TOK, 16)], meta_pair.at[core])
    for g in range(8):
        at = pl.multiple_of((2 * g + 1 - core) * 256, 256)
        to_partner(hid.at[:, pl.ds(at, 256)], hid_partner.at[:, pl.ds(g * 256, 256)])
    q_pair[core] = q[...]
    do_pair[core] = do[...]
    tables_pair[core] = tables[...]
    meta_pair[core] = kv[0, TOK : TOK + 16]
    for k in range(3):
        lines[k].forward()
    for k in range(3):
        lines[k].finish()
        planes[k].start()
        spaces[k][0].start()
    for k in range(3):
        planes[k].forward()
        spaces[k][1].start()
        spaces[k][2].start()
    for k in range(3):
        spaces[k][0].forward()
    for k in range(3):
        planes[k].finish()
        spaces[k][3].start()
    for n in range(1, 4):
        for k in range(3):
            spaces[k][n].forward()
    for n in range(4):
        for k in range(3):
            spaces[k][n].finish()
    for copy in waits:
        copy.wait_send()
    for copy in pair:
        copy.wait()


def gather(kv, q, do, tables, hid):
    n_pair = 12
    return pl.pallas_call(
        gather_kernel,
        out_shape=(
            jax.ShapeDtypeStruct((2, 4, 4, 2, 2, KV_ROWS, HD), BF16),
            jax.ShapeDtypeStruct((2, *q.shape), BF16),
            jax.ShapeDtypeStruct((2, *do.shape), BF16),
            jax.ShapeDtypeStruct((2, *tables.shape), F32),
            jax.ShapeDtypeStruct((2, 16, HD), BF16),
            jax.ShapeDtypeStruct((TOK, 2048), BF16),
        ),
        in_specs=[*in_vmem(4), pl.BlockSpec(memory_space=pl.ANY)],
        out_specs=(*in_vmem(5), pl.BlockSpec(memory_space=pl.ANY)),
        scratch_shapes=[
            pltpu.SemaphoreType.DMA((3, 6, 4)),
            pltpu.SemaphoreType.DMA((3, 6, 4)),
            pltpu.SemaphoreType.DMA((n_pair,)),
            pltpu.SemaphoreType.DMA((n_pair,)),
        ],
        compiler_params=params(0),
        name="gather_kv",
    )(kv, q, do, tables, hid)


def unit_loop(fixed, body):
    dims = left_dims(fixed)
    count = math.prod(dims)
    if count == 1:
        body(())
        return

    def step(i, carry):
        index, rest = [], i
        for size in reversed(dims):
            index.append(rest % size)
            rest = rest // size
        body(tuple(reversed(index)))
        return carry

    lax.fori_loop(0, count, step, 0)


def ring_slots(tails):
    shapes = []
    for (a, b, c), tail in zip(ORDERS, tails):
        dims = left_dims((a, b))
        shapes.append(pltpu.VMEM((4, 6, *dims, *tail), BF16))
        shapes.append(pltpu.VMEM((6, *dims, *tail), BF16))
        shapes.append(pltpu.VMEM((6, *tail), BF16))
    return shapes


class Collect:
    def __init__(self, me, axis, fixed, x, subs, buf, send, recv, waits):
        self.me, self.axis, self.fixed, self.x, self.subs = me, axis, fixed, x, subs
        self.buf, self.send, self.recv, self.waits = buf, send, recv, waits
        self.copies = {}

    def chunks(self, delta, half):
        value = (self.me[self.axis] + delta) % 4
        return self.x.at[(*place({**self.fixed, self.axis: value}), *self.subs(half))]

    def post(self, message, bound, half, delta):
        copy = remote(
            self.chunks(bound, half),
            self.buf.at[message],
            (self.send.at[message], self.recv.at[message]),
            along(self.axis, (self.me[self.axis] + delta) % 4),
        )
        copy.start()
        self.waits.append(copy)
        self.copies[message] = copy

    def start_far(self):
        self.post(0, 2, 0, 1)
        self.post(3, 2, 1, 3)

    def start_right(self):
        self.post(1, 1, 1, 1)

    def start_left(self):
        self.post(4, 3, 0, 3)

    def start(self):
        self.start_far()
        self.start_right()
        self.start_left()

    def add(self, delta, half, messages, finish=None):
        for message in messages:
            self.copies[message].wait_recv()
        ref = self.chunks(delta, half)
        buf = self.buf

        def body(index):
            whole = (*index, slice(None), slice(None))
            total = ref[whole].astype(F32)
            for message in messages:
                total = total + buf[(message, *whole)].astype(F32)
            if finish is None:
                ref[whole] = total.astype(BF16)
            else:
                finish(half, total)

        unit_loop({**self.fixed, self.axis: 0}, body)

    def forward(self):
        self.add(1, 0, (0,))
        self.post(2, 1, 0, 1)
        self.add(3, 1, (3,))
        self.post(5, 3, 1, 3)

    def collect(self, finish=None):
        self.add(0, 1, (1, 5), finish)
        self.add(0, 0, (4, 2), finish)


def reduce_to_own(me, x, slots, subs, send, recv, finish, meanwhile=None):
    waits = []
    first, second, third = [], [], []
    for k, (a, b, c) in enumerate(ORDERS):
        mine = functools.partial(subs, k)
        one, two, three = slots[3 * k : 3 * k + 3]
        first.append(
            [
                Collect(
                    me, a, {b: (me[b] + off) % 4}, x, mine, one.at[n], send.at[k, n], recv.at[k, n], waits
                )
                for n, off in enumerate((2, 1, 3, 0))
            ]
        )
        second.append(Collect(me, b, {a: me[a]}, x, mine, two, send.at[k, 4], recv.at[k, 4], waits))
        third.append(
            Collect(me, c, {a: me[a], b: me[b]}, x, mine, three, send.at[k, 5], recv.at[k, 5], waits)
        )
    colours = range(3)
    for n in range(2):
        for k in colours:
            first[k][n].start()
    if meanwhile is not None:
        meanwhile()
    for k in colours:
        first[k][0].forward()
    for k in colours:
        first[k][2].start()
    for k in colours:
        first[k][1].forward()
    for k in colours:
        first[k][3].start()
    for k in colours:
        first[k][0].collect()
        second[k].start_far()
    for k in colours:
        first[k][2].forward()
    for k in colours:
        first[k][1].collect()
        second[k].start_right()
    for k in colours:
        first[k][3].forward()
    for k in colours:
        first[k][2].collect()
        second[k].start_left()
    for k in colours:
        second[k].forward()
    for k in colours:
        first[k][3].collect()
    for k in colours:
        second[k].collect()
        third[k].start()
    for k in colours:
        third[k].forward()
    for k in colours:
        third[k].collect(functools.partial(finish, k))
    for copy in waits:
        copy.wait_send()


DKV_PARTS = ((0, 48), (48, 48), (96, 32))


def scatter_kv_kernel(
    part, dq, dq_pair, dkv_pair, x, dq_in, *rest
):
    slots, (send, recv, pair_send, pair_recv, load_sem) = rest[:9], rest[9:]
    me = here()
    core = lax.axis_index("c")
    other = {"c": 1 - core}
    load = pltpu.make_async_copy(part, x, load_sem)
    load.start()
    enter(me)
    load.wait()
    first = remote(dq.at[1 - core], dq_in, (pair_send.at[0], pair_recv.at[0]), other)
    first.start()

    def subs(k, half):
        return (half, pl.ds(*DKV_PARTS[k]), slice(None))

    def finish(k, half, value):
        dkv_pair[(core, half, pl.ds(*DKV_PARTS[k]))] = value

    second = remote(
        dq_pair.at[core], dq_pair.at[core], (pair_send.at[1], pair_recv.at[1]), other
    )

    def meanwhile():
        first.wait()
        dq_pair[core] = dq[core] + dq_in[...]
        second.start()

    reduce_to_own(me, x, slots, subs, send, recv, finish, meanwhile)
    third = remote(
        dkv_pair.at[core], dkv_pair.at[core], (pair_send.at[2], pair_recv.at[2]), other
    )
    third.start()
    second.wait()
    third.wait()


def scatter_kv(part, dq):
    return pl.pallas_call(
        scatter_kv_kernel,
        out_shape=(
            jax.ShapeDtypeStruct(dq.shape, F32),
            jax.ShapeDtypeStruct((2, 2, TOK, HD), F32),
        ),
        in_specs=[pl.BlockSpec(memory_space=pl.ANY), *in_vmem(1)],
        out_specs=tuple(in_vmem(2)),
        scratch_shapes=[
            pltpu.VMEM(part.shape, BF16),
            pltpu.VMEM(dq.shape[1:], F32),
            *ring_slots([(n, HD) for _, n in DKV_PARTS]),
            pltpu.SemaphoreType.DMA((3, 6, 6)),
            pltpu.SemaphoreType.DMA((3, 6, 6)),
            pltpu.SemaphoreType.DMA((3,)),
            pltpu.SemaphoreType.DMA((3,)),
            pltpu.SemaphoreType.DMA,
        ],
        compiler_params=params(2),
        name="scatter_kv",
    )(part, dq)


def scatter_weights_kernel(part, out, x, *rest):
    slots, (send, recv, load_sem) = rest[:9], rest[9:]
    me = here()
    load = pltpu.make_async_copy(part, x, load_sem)
    load.start()
    enter(me, partner=False)
    load.wait()

    def columns(k, half):
        return pl.ds((2 * k + half) * 128, 128)

    def subs(k, half):
        return (slice(None), columns(k, half))

    def finish(k, half, value):
        out[(slice(None), columns(k, half))] = value

    reduce_to_own(me, x, slots, subs, send, recv, finish)


def scatter_weights(part):
    return pl.pallas_call(
        scatter_weights_kernel,
        out_shape=jax.ShapeDtypeStruct(part.shape[4:], F32),
        in_specs=[pl.BlockSpec(memory_space=pl.ANY)],
        out_specs=in_vmem(1)[0],
        scratch_shapes=[
            pltpu.VMEM(part.shape, BF16),
            *ring_slots([(32, 128)] * 3),
            pltpu.SemaphoreType.DMA((3, 6, 6)),
            pltpu.SemaphoreType.DMA((3, 6, 6)),
            pltpu.SemaphoreType.DMA,
        ],
        compiler_params=params(3),
        name="scatter_weights",
    )(part)


def swap_kernel(a, b, a_in, b_in, send, recv):
    other = {"c": 1 - lax.axis_index("c")}
    enter(None, ring=False)
    one = remote(a, a_in, (send.at[0], recv.at[0]), other)
    two = remote(b, b_in, (send.at[1], recv.at[1]), other)
    one.start()
    two.start()
    one.wait()
    two.wait()


def swap(a, b):
    return pl.pallas_call(
        swap_kernel,
        out_shape=(jax.ShapeDtypeStruct(a.shape, a.dtype), jax.ShapeDtypeStruct(b.shape, b.dtype)),
        in_specs=in_vmem(2),
        out_specs=tuple(in_vmem(2)),
        scratch_shapes=[pltpu.SemaphoreType.DMA((2,)), pltpu.SemaphoreType.DMA((2,))],
        compiler_params=params(1),
        name="swap_partials",
    )(a, b)


KEYS = 256
CHUNKS = 16


def dot_nt(a, b):
    return lax.dot_general(a, b, (((1,), (1,)), ((), ())), preferred_element_type=F32)


def dot_nn(a, b):
    return lax.dot_general(a, b, (((1,), (0,)), ((), ())), preferred_element_type=F32)


def dot_tn(a, b):
    return lax.dot_general(a, b, (((0,), (0,)), ((), ())), preferred_element_type=F32)


def by_run(dst, src, d):
    for run in range(2):
        for h in range(HQ):
            dst[run, d, h * 64 : (h + 1) * 64, :] = src[
                d, run * 64 : (run + 1) * 64, h * HD : (h + 1) * HD
            ]


def edge_of(table, d):
    return jnp.minimum(table[128 + d] // 4, CHUNKS - 1)


def aside(edge, j):
    sel = (j >= edge).astype(jnp.int32)
    return sel, j + sel


def run_start(a, sel):
    return (a if sel == 0 else 255 - a) * 64


def chunk(ref, *index):
    return ref[(*index[:-1], pl.ds(4 * index[-1], 4))].reshape(KEYS, HD)


def forward_kernel(
    table, kv, q, ks, vs, o, lse, dense_scores, edge_scores, qs, top, total
):
    def put(b, carry):
        r = table[b]
        ks[0, r] = kv[b, 0, 0:64]
        ks[1, r] = kv[b, 0, 64:128]
        vs[0, r] = kv[b, 1, 0:64]
        vs[1, r] = kv[b, 1, 64:128]
        return carry

    lax.fori_loop(0, CHIPS, put, 0, unroll=4)
    for d in range(2):
        by_run(qs, q, d)
    top[...] = jnp.full_like(top, -1e29)
    total[...] = jnp.zeros_like(total)
    o[...] = jnp.zeros_like(o)

    lane = lax.broadcasted_iota(jnp.int32, (1, KEYS), 1)
    row = lax.broadcasted_iota(jnp.int32, (256, KEYS), 0) % 64
    edges = [edge_of(table, d) for d in range(2)]

    def dense(it, carry):
        s = dot_nt(qs[1].reshape(512, HD), chunk(ks, 0, it))
        dense_scores[it] = s
        top[1] = jnp.maximum(top[1], jnp.maximum(s[:, :HD], s[:, HD:]).reshape(2, 256, HD))
        return carry

    def plain(j, carry):
        for d in range(2):
            sel, ch = aside(edges[d], j)
            s = dot_nt(qs[sel, d], chunk(ks, sel, ch))
            edge_scores[d, j] = s
            top[sel, d] = jnp.maximum(top[sel, d], jnp.maximum(s[:, :HD], s[:, HD:]))
        return carry

    lax.fori_loop(0, CHUNKS, dense, 0, unroll=2)
    lax.fori_loop(0, CHUNKS - 1, plain, 0, unroll=3)
    for d in range(2):
        for sel in range(2):
            s = dot_nt(qs[sel, d], chunk(ks, sel, edges[d]))
            own = run_start(table[130 + d], sel)
            starts = [run_start(table[64 + 4 * edges[d] + r], sel) - own for r in range(4)]
            offset = jnp.where(
                lane < 128,
                jnp.where(lane < 64, starts[0], starts[1]),
                jnp.where(lane < 192, starts[2], starts[3]),
            ) + lane % 64
            s = jnp.where(offset <= row, s, masked_score)
            edge_scores[d, CHUNKS - 1 + sel] = s
            top[sel, d] = jnp.maximum(top[sel, d], jnp.maximum(s[:, :HD], s[:, HD:]))

    factor = SCALE * LOG2E
    for d in range(2):
        for sel in range(2):
            peak = jnp.max(top[sel, d], axis=1, keepdims=True)
            top[sel, d] = jnp.broadcast_to(peak * factor, (256, HD))

    def weights(s, peak):
        p0 = jnp.exp2(s[:, :HD] * factor - peak)
        p1 = jnp.exp2(s[:, HD:] * factor - peak)
        return p0 + p1, jnp.concatenate([p0.astype(BF16), p1.astype(BF16)], axis=1)

    def dense_out(it, carry):
        both, p = weights(dense_scores[it], top[1].reshape(512, HD))
        total[1] += both.reshape(2, 256, HD)
        o[1] += dot_nn(p, chunk(vs, 0, it)).reshape(2, 256, HD)
        return carry

    def edge_out(d, j, sel, ch):
        both, p = weights(edge_scores[d, j], top[sel, d])
        total[sel, d] += both
        o[sel, d] += dot_nn(p, chunk(vs, sel, ch))

    def plain_out(j, carry):
        for d in range(2):
            edge_out(d, j, *aside(edges[d], j))
        return carry

    lax.fori_loop(0, CHUNKS, dense_out, 0, unroll=2)
    lax.fori_loop(0, CHUNKS - 1, plain_out, 0, unroll=3)
    for d in range(2):
        for sel in range(2):
            edge_out(d, CHUNKS - 1 + sel, sel, edges[d])

    for d in range(2):
        for sel in range(2):
            summed = jnp.sum(total[sel, d], axis=1, keepdims=True)
            some = summed > 0.0
            safe = jnp.where(some, summed, 1.0)
            o[sel, d] = o[sel, d] / safe
            level = top[sel, d] * (1.0 / LOG2E) + jnp.log(safe)
            lse[sel, d] = jnp.where(some, level, masked_score)


def forward(table, kv, q):
    sorted_shape = jax.ShapeDtypeStruct((2, CHIPS, 64, HD), BF16)
    rows = jax.ShapeDtypeStruct((2, 2, 256, HD), F32)
    return pl.pallas_call(
        forward_kernel,
        out_shape=(sorted_shape, sorted_shape, rows, rows),
        in_specs=[pl.BlockSpec(memory_space=pltpu.SMEM), *in_vmem(2)],
        out_specs=tuple(in_vmem(4)),
        scratch_shapes=[
            pltpu.VMEM((CHUNKS, 512, KEYS), F32),
            pltpu.VMEM((2, CHUNKS + 1, 256, KEYS), F32),
            pltpu.VMEM((2, 2, 256, HD), BF16),
            pltpu.VMEM((2, 2, 256, HD), F32),
            pltpu.VMEM((2, 2, 256, HD), F32),
        ],
        compiler_params=params(),
        name="attention_forward",
    )(table, kv, q)


def backward_kernel(
    table, ks, vs, q, do, o, lse, o_in, lse_in,
    attended, part, dq,
    qs, dos, level, delta, final, grads, dqs,
):
    for d in range(2):
        by_run(qs, q, d)
        by_run(dos, do, d)
        for sel in range(2):
            one, two = lse[sel, d], lse_in[sel, d]
            most = jnp.maximum(one, two)
            w1, w2 = jnp.exp(one - most), jnp.exp(two - most)
            both = w1 + w2
            out = (o[sel, d] * w1 + o_in[sel, d] * w2) / both
            final[sel, d] = out
            logs = (most + jnp.log(both)) * LOG2E
            level[sel, d] = jnp.transpose(logs)[0:8]
            dots = jnp.sum(dos[sel, d].astype(F32) * out, axis=1, keepdims=True)
            delta[sel, d] = jnp.transpose(jnp.broadcast_to(dots, (256, HD)))[0:8]
    core = table[132]
    for run in range(2):
        for h in range(HQ):
            attended[run * 64 : (run + 1) * 64, h * HD : (h + 1) * HD] = final[
                run, core, h * 64 : (h + 1) * 64, :
            ].astype(BF16)

    dqs[...] = jnp.zeros_like(dqs)

    def clear(i, carry):
        for sel in range(2):
            for which in range(2):
                grads[sel, which, i] = jnp.zeros((64, HD), F32)
        return carry

    lax.fori_loop(0, CHIPS, clear, 0, unroll=4)

    factor = SCALE * LOG2E
    edges = [edge_of(table, d) for d in range(2)]

    def terms(k, v, qq, gg, lev, dl, mask=None):
        p = jnp.exp2(dot_nt(k, qq) * factor - lev)
        if mask is not None:
            p = mask(p)
        ds = p * (dot_nt(v, gg) - dl)
        return p.astype(BF16), ds.astype(BF16)

    def collect(ksel, ch, p, ds, qq, gg):
        spot = pl.ds(4 * ch, 4)
        grads[ksel, 0, spot] += dot_nn(ds, qq).reshape(4, 64, HD)
        grads[ksel, 1, spot] += dot_nn(p, gg).reshape(4, 64, HD)

    def dense(it, carry):
        k, v = chunk(ks, 0, it), chunk(vs, 0, it)
        qq, gg = qs[1].reshape(512, HD), dos[1].reshape(512, HD)
        lev = jnp.concatenate([level[1, 0, 0:1], level[1, 1, 0:1]], axis=1)
        dl = jnp.concatenate([delta[1, 0, 0:1], delta[1, 1, 0:1]], axis=1)
        p, ds = terms(k, v, qq, gg, lev, dl)
        collect(0, it, p, ds, qq, gg)
        dqs[1] += dot_tn(ds, k).reshape(2, 256, HD)
        return carry

    def one(d, sel, ch, mask=None):
        k, v = chunk(ks, sel, ch), chunk(vs, sel, ch)
        qq, gg = qs[sel, d], dos[sel, d]
        p, ds = terms(k, v, qq, gg, level[sel, d, 0:1], delta[sel, d, 0:1], mask)
        return sel, ch, k, qq, gg, p, ds

    def gather_in(d, sel, ch, k, qq, gg, p, ds):
        collect(sel, ch, p, ds, qq, gg)
        dqs[sel, d] += dot_tn(ds, k)

    def plain(j, carry):
        found = [one(d, *aside(edges[d], j)) for d in range(2)]
        for d in range(2):
            gather_in(d, *found[d])
        return carry

    lax.fori_loop(0, CHUNKS, dense, 0, unroll=2)
    lax.fori_loop(0, CHUNKS - 1, plain, 0, unroll=3)

    difference = (
        lax.broadcasted_iota(jnp.int32, (64, 256), 1) % 64
        - lax.broadcasted_iota(jnp.int32, (64, 256), 0)
    )
    for d in range(2):
        for sel in range(2):
            own = run_start(table[130 + d], sel)

            def mask(p, d=d, sel=sel, own=own):
                pieces = []
                for r in range(4):
                    least = run_start(table[64 + 4 * edges[d] + r], sel) - own
                    pieces.append(
                        jnp.where(difference >= least, p[64 * r : 64 * (r + 1)], 0.0)
                    )
                return jnp.concatenate(pieces, axis=0)

            gather_in(d, *one(d, sel, edges[d], mask))

    for d in range(2):
        for sel in range(2):
            dq[d, sel] = dqs[sel, d] * SCALE

    def put(b, carry):
        r = table[b]
        for sel in range(2):
            part[b, 0, 64 * sel : 64 * (sel + 1)] = (grads[sel, 0, r] * SCALE).astype(BF16)
            part[b, 1, 64 * sel : 64 * (sel + 1)] = grads[sel, 1, r].astype(BF16)
        return carry

    lax.fori_loop(0, CHIPS, put, 0, unroll=4)


def backward(table, ks, vs, q, do, o, lse, o_in, lse_in):
    return pl.pallas_call(
        backward_kernel,
        out_shape=(
            jax.ShapeDtypeStruct((TOK, HQ * HD), BF16),
            jax.ShapeDtypeStruct((CHIPS, 2, TOK, HD), BF16),
            jax.ShapeDtypeStruct((2, 2, 256, HD), F32),
        ),
        in_specs=[pl.BlockSpec(memory_space=pltpu.SMEM), *in_vmem(8)],
        out_specs=tuple(in_vmem(3)),
        scratch_shapes=[
            pltpu.VMEM((2, 2, 256, HD), BF16),
            pltpu.VMEM((2, 2, 256, HD), BF16),
            pltpu.VMEM((2, 2, 8, 256), F32),
            pltpu.VMEM((2, 2, 8, 256), F32),
            pltpu.VMEM((2, 2, 256, HD), F32),
            pltpu.VMEM((2, 2, CHIPS, 64, HD), F32),
            pltpu.VMEM((2, 2, 256, HD), F32),
        ],
        compiler_params=params(),
        name="attention_backward",
    )(table, ks, vs, q, do, o, lse, o_in, lse_in)


def turned(u, cosine, sine):
    return u * cosine + pltpu.roll(u, 64, 1) * sine


def tail_kernel(
    table, dq, dkv, tables, hidden, hid_in, wq, wk, wv,
    hidden_grad, part,
    grads, hid, wq_in, wk_in, wv_in, sems,
):
    core = table[132]
    loads = []

    def load(src, dst):
        copy = pltpu.make_async_copy(src, dst, sems.at[len(loads)])
        copy.start()
        loads.append(copy)

    for g in range(8):
        at = pl.multiple_of((2 * g + core) * 256, 256)
        load(hidden.at[:, pl.ds(at, 256)], hid.at[pl.ds(0, TOK), pl.ds(g * 256, 256)])
    load(hid_in, hid.at[pl.ds(TOK, TOK)])
    load(wq, wq_in)
    load(wk, wk_in)
    load(wv, wv_in)

    for n in range(2):
        d = core if n == 0 else 1 - core
        base = n * TOK
        for run in range(2):
            rows = slice(run * 64, (run + 1) * 64)
            cosine, sine = tables[d, 0, rows], tables[d, 1, rows]
            for h in range(HQ):
                g = turned(dq[d, run, h * 64 : (h + 1) * 64], cosine, sine)
                grads[base + run * 64 : base + (run + 1) * 64, h * HD : (h + 1) * HD] = g.astype(BF16)
        gk = turned(dkv[d, 0], tables[d, 0], tables[d, 1])
        grads[base : base + TOK, 512:640] = gk.astype(BF16)
        grads[base : base + TOK, 640:768] = dkv[d, 1].astype(BF16)

    for copy in loads[:9]:
        copy.wait()
    for g in range(8):
        block = dot_tn(hid[:, g * 256 : (g + 1) * 256], grads[...])
        part[g // 4, g % 4] = block.astype(BF16).reshape(4, 2, 32, 768)
    for copy in loads[9:]:
        copy.wait()

    def columns(n, carry):
        rows = pl.ds(pl.multiple_of(n * 256, 256), 256)
        both = jnp.concatenate([wk_in[rows], wv_in[rows]], axis=1)
        block = dot_nt(grads[0:TOK, 0:512], wq_in[rows]) + dot_nt(grads[0:TOK, 512:768], both)
        hidden_grad[:, rows] = block.astype(BF16)
        return carry

    lax.fori_loop(0, 16, columns, 0, unroll=2)


def tail(table, dq, dkv, tables, hidden, hid_in, wq, wk, wv):
    return pl.pallas_call(
        tail_kernel,
        out_shape=(
            jax.ShapeDtypeStruct((TOK, 4096), BF16),
            jax.ShapeDtypeStruct((2, 4, 4, 2, 32, 768), BF16),
        ),
        in_specs=[
            pl.BlockSpec(memory_space=pltpu.SMEM),
            *in_vmem(3),
            *[pl.BlockSpec(memory_space=pl.ANY)] * 5,
        ],
        out_specs=tuple(in_vmem(2)),
        scratch_shapes=[
            pltpu.VMEM((2 * TOK, 768), BF16),
            pltpu.VMEM((2 * TOK, 2048), BF16),
            pltpu.VMEM(wq.shape, BF16),
            pltpu.VMEM(wk.shape, BF16),
            pltpu.VMEM(wv.shape, BF16),
            pltpu.SemaphoreType.DMA((12,)),
        ],
        compiler_params=params(),
        name="token_grads",
    )(table, dq, dkv, tables, hidden, hid_in, wq, wk, wv)


def project_kernel(
    first, hidden, tables, wq, wk, wv, kv, q, acc, hid, wq_in, wk_in, wv_in, sems
):
    copies = []
    for n in range(4):
        rows = pl.ds(n * 1024, 1024)
        group = []
        for src, dst in (
            (hidden.at[:, rows], hid.at[:, rows]),
            (wq.at[rows], wq_in.at[rows]),
            (wk.at[rows], wk_in.at[rows]),
            (wv.at[rows], wv_in.at[rows]),
        ):
            copy = pltpu.make_async_copy(src, dst, sems.at[n, len(group)])
            copy.start()
            group.append(copy)
        copies.append(group)
    for n in range(4):
        for copy in copies[n]:
            copy.wait()
        rows = slice(n * 1024, (n + 1) * 1024)
        h = hid[:, rows]
        both = jnp.concatenate([wk_in[rows], wv_in[rows]], axis=1)
        left, right = dot_nn(h, wq_in[rows]), dot_nn(h, both)
        if n == 0:
            acc[:, :512] = left
            acc[:, 512:] = right
        else:
            acc[:, :512] += left
            acc[:, 512:] += right
    cosine, sine = tables[0], tables[1]

    def rotated(u):
        return (u * cosine - pltpu.roll(u, 64, 1) * sine).astype(BF16)

    for h in range(HQ):
        q[:, h * HD : (h + 1) * HD] = rotated(acc[:, h * HD : (h + 1) * HD])
    kv[0, 0:TOK] = rotated(acc[:, 512:640])
    kv[1, 0:TOK] = acc[:, 640:768].astype(BF16)
    index = (first[0] // 64).astype(F32)
    for n in range(2):
        kv[n, TOK:KV_ROWS] = jnp.full((16, HD), index, F32).astype(BF16)


def project(first, hidden, tables, wq, wk, wv):
    anywhere = pl.BlockSpec(memory_space=pl.ANY)
    return pl.pallas_call(
        project_kernel,
        out_shape=(
            jax.ShapeDtypeStruct((2, KV_ROWS, HD), BF16),
            jax.ShapeDtypeStruct((TOK, HQ * HD), BF16),
        ),
        in_specs=[
            pl.BlockSpec(memory_space=pltpu.SMEM), anywhere, *in_vmem(1), anywhere, anywhere, anywhere
        ],
        out_specs=tuple(in_vmem(2)),
        scratch_shapes=[
            pltpu.VMEM((TOK, 768), F32),
            pltpu.VMEM(hidden.shape, BF16),
            pltpu.VMEM(wq.shape, BF16),
            pltpu.VMEM(wk.shape, BF16),
            pltpu.VMEM(wv.shape, BF16),
            pltpu.SemaphoreType.DMA((4, 4)),
        ],
        compiler_params=params(),
        name="project",
    )(first, hidden, tables, wq, wk, wv)


def shards(hidden, position, query_weight, key_weight, value_weight, output_grad):
    core = lax.axis_index("c")
    angles = position.astype(F32)[:, None] * frequencies(HD)[None, :]
    cosine, sine = jnp.cos(angles), jnp.sin(angles)
    cos2 = jnp.concatenate([cosine, cosine], axis=1)
    sin2 = jnp.concatenate([sine, -sine], axis=1)
    tables = jnp.stack([cos2, sin2])

    kv, q = project(position[:1], hidden, tables, query_weight, key_weight, value_weight)
    kv_all, q_pair, do_pair, tables_pair, meta_pair, hid_in = gather(
        kv, q, output_grad, tables, hidden
    )
    kv_all = kv_all.reshape(CHIPS, 2, KV_ROWS, HD)
    runs = kv_all[:, 0, TOK, 0].astype(jnp.int32)
    below = (runs[None, :] < runs[:, None]).astype(jnp.int32)
    rank = jnp.sum(below, axis=1)
    slots = lax.iota(jnp.int32, CHIPS)
    rising = jnp.sum(jnp.where(rank[None, :] == slots[:, None], runs[None, :], 0), axis=1)
    own = meta_pair[:, 0, 0].astype(jnp.int32)
    count = jnp.sum((runs[None, :] < own[:, None]).astype(jnp.int32), axis=1)
    table = jnp.concatenate(
        [rank, rising, count, own, core[None].astype(jnp.int32), jnp.zeros((3,), jnp.int32)]
    )

    ks, vs, o, lse = forward(table, kv_all, q_pair)
    o_in, lse_in = swap(o, lse)
    attended, part, dq = backward(table, ks, vs, q_pair, do_pair, o, lse, o_in, lse_in)
    dq_pair, dkv_pair = scatter_kv(part.reshape(2, 4, 4, 2, 2, TOK, HD), dq)
    hidden_grad, weights = tail(
        table, dq_pair, dkv_pair, tables_pair, hidden, hid_in, query_weight, key_weight, value_weight
    )
    total = scatter_weights(weights)
    return attended, hidden_grad, total[:, :512], total[:, 512:640], total[:, 640:]


def solution(mesh):
    split = Mesh(mesh.devices.reshape(2, 4, 2, 4, 2), AXES)
    rows = P(AXES, None)
    return jax.shard_map(
        shards,
        mesh=split,
        in_specs=(rows, P(AXES), P(), P(), P(), rows),
        out_specs=(rows,) * 5,
        check_vma=False,
    )
```
